32 devices in a mesh: group: 2 (over y), seq: 4 (over z), blk: 2 (over x), tp: 2 (over core).
Axes of the slice: x: 2, y: 2, z: 4, core: 2. Of those that a mesh axis runs over, the one named last changes fastest.
Arguments:
- tokens: bfloat16 [2048, 3072], P(('group', 'blk'), ('seq', 'tp')), parts along dimension 0, may hold values from -64 to 64
- timestep: int32 [2], P('group'), parts along dimension 0, may hold values from 25 to 49
- padded_heads: int32 [2], P('group'), parts along dimension 0, may hold values from 1 to 3
- modulation: float32 [50, 3, 3072], replicated, may hold values from -3 to 3
- qkv_weight: bfloat16 [3, 3072, 1024], P(None, 'blk', ('seq', 'tp')), may hold values from -1 to 1
- out_weight: bfloat16 [1024, 3072], P(('seq', 'tp'), 'blk'), may hold values from -0.5 to 0.5
Outputs:
- update: bfloat16 [2048, 3072], P(('group', 'blk'), ('seq', 'tp')), parts along dimension 0
The draws below stay inside these ranges and needn't reach their ends.
There are 2 independent parts, one for each index of `group`. The reference program is written for one: setup_inputs(seed, part) draws one part's arguments, and reference() takes and returns one part's arrays. A program takes and returns all parts, laid end to end along the dimension named above; an argument that names none is the same for every part. Nothing has to cross between parts.
All inputs are finite; a program needn't handle non-finite values.
Results may differ from the reference program's by a relative error of at most 0.023.
Values may be sent and summed in bfloat16 or wider, within the bound.
No kernel may reach another device: no remote copies, remote signals or barrier semaphores. Data moves between devices by JAX's collectives and lax.ppermute only.
A program may use at most 64 MiB of HBM per device.

```python
import math
import jax
import jax.numpy as jnp
from jax import lax

D = 3072
E = 128
STEPS = 50
HEADS = 8
TOKENS = 1024


def draw_tokens(key, part):
    noise_key = jax.random.fold_in(key, 0)
    column_key = jax.random.fold_in(key, 1)
    mean_key = jax.random.fold_in(key, 3)
    column = jnp.arange(D, dtype=jnp.float32) / max(D - 1, 1)
    rising = jnp.exp(math.log(3.0) * column) * jax.random.uniform(column_key, (D,), jnp.float32, 0.7, 1.4)
    noise = jax.random.normal(noise_key, (TOKENS, D), jnp.float32)
    offset = 0.5 * jax.random.normal(mean_key, (TOKENS, 1), jnp.float32)
    result = (noise + offset) * rising
    return jnp.clip(result, -64.0, 64.0).astype(jnp.bfloat16)


def draw_qkv_weight(key, part):
    noise_key = jax.random.fold_in(key, 0)
    sigma = 1.2 / math.sqrt(D)
    result = jax.random.normal(noise_key, (3, D, HEADS * E), jnp.float32) * sigma
    return jnp.clip(result, -1.0, 1.0).astype(jnp.bfloat16)


def shard_levels(rng, shape, cuts, low, high):
    factor_of = 1.0
    for dim, shards_of in cuts:
        draws = jax.random.uniform(jax.random.fold_in(jax.random.fold_in(rng, 6), dim), (shards_of,), jnp.float32, low / len(cuts), high / len(cuts))
        factor_of = factor_of * jnp.repeat(jnp.exp(draws), shape[dim] // shards_of).reshape((-1,) + (1,) * (len(shape) - 1 - dim))
    return factor_of


def centred(own_key, extent, deviation, most, cuts=(), kind=jnp.bfloat16):
    values = jax.random.normal(own_key, extent, jnp.float32) * deviation
    if len(cuts) > 0:
        values = shard_levels(own_key, extent, cuts, -0.22, 0.18) * values
    return jnp.clip(values, min=-most, max=most).astype(kind)


def setup_inputs(seed: int = 0, part: int = 0) -> dict:
    seeds = jax.random.split(jax.random.key(seed), 7)
    part_splits = jax.random.split(jax.random.fold_in(seeds[6], part), 7)
    return {
        "tokens": draw_tokens(jax.random.fold_in(jax.random.fold_in(seeds[6], part), 71), part),
        "timestep": jax.random.randint(part_splits[1], (1,), STEPS // 2, STEPS).astype(jnp.int32),
        "padded_heads": jax.random.randint(part_splits[2], (1,), HEADS // 8, HEADS * 3 // 8 + 1).astype(jnp.int32),
        "modulation": centred(seeds[3], (STEPS, 3, D), 0.5, 3.0, (), jnp.float32),
        "qkv_weight": draw_qkv_weight(jax.random.fold_in(seeds[6], 71), part),
        "out_weight": centred(seeds[5], (HEADS * E, D), E ** -0.5, 0.5, ((0, 8), (1, 2))),
    }


epsilon = 1e-06

def reference(tokens, timestep, padded_heads, modulation, qkv_weight, out_weight):
    table_row = lax.dynamic_index_in_dim(modulation, timestep[0], 0, keepdims=False)
    values = tokens.astype(jnp.float32)
    average = lax.optimization_barrier(jnp.mean(values, axis=1, keepdims=True))
    centered = values - average
    spread = lax.optimization_barrier(jnp.mean(centered * centered, axis=1, keepdims=True))
    normed = centered * lax.rsqrt(spread + epsilon)
    modulated = (normed * (1.0 + table_row[1]) + table_row[0]).astype(jnp.bfloat16)
    queries = jnp.dot(modulated, qkv_weight[0], preferred_element_type=jnp.float32).astype(jnp.bfloat16)
    keys_all = jnp.dot(modulated, qkv_weight[1], preferred_element_type=jnp.float32).astype(jnp.bfloat16)
    values_all = jnp.dot(modulated, qkv_weight[2], preferred_element_type=jnp.float32).astype(jnp.bfloat16)
    live_heads = HEADS - padded_heads[0]
    factor = 1.0 / math.sqrt(E)

    def one_head(running, head_index):
        query_head = lax.dynamic_slice_in_dim(queries, head_index * E, E, 1)
        key_head = lax.dynamic_slice_in_dim(keys_all, head_index * E, E, 1)
        value_head = lax.dynamic_slice_in_dim(values_all, head_index * E, E, 1)
        scores = lax.dot_general(query_head, key_head, (((1,), (1,)), ((), ())), preferred_element_type=jnp.float32) * factor
        largest = lax.optimization_barrier(jnp.max(scores, axis=1, keepdims=True))
        weights = jnp.exp(scores - largest)
        totals = lax.optimization_barrier(jnp.sum(weights, axis=1, keepdims=True))
        attended = jnp.dot(weights.astype(jnp.bfloat16), value_head, preferred_element_type=jnp.float32) / totals
        masked = jnp.where(head_index < live_heads, attended, 0.0).astype(jnp.bfloat16)
        out_rows = lax.dynamic_slice_in_dim(out_weight, head_index * E, E, 0)
        head_term = jnp.dot(masked, out_rows, preferred_element_type=jnp.float32).astype(jnp.bfloat16)
        head_term = lax.optimization_barrier(head_term).astype(jnp.float32)
        return (running + head_term, None)
    summed, ignored = lax.scan(one_head, jnp.zeros((TOKENS, D), jnp.float32), jnp.arange(HEADS, dtype=jnp.int32))
    return (table_row[2] * summed).astype(jnp.bfloat16)
```

```python
import functools
import math

import jax
import jax.numpy as jnp
import numpy as np
from jax import lax
from jax.experimental import pallas as pl
from jax.experimental.pallas import tpu as pltpu
from jax.sharding import PartitionSpec as P

epsilon = 1e-06
ANY = pl.BlockSpec(memory_space=pl.ANY)
VMEM = pl.BlockSpec(memory_space=pltpu.VMEM)
SMEM = pl.BlockSpec(memory_space=pltpu.SMEM)


def folded_order(count):
    return list(range(1, count, 2)) + list(range(0, count, 2))[::-1]


def ring_pairs(order, step=1):
    count = len(order)
    return [(order[i], order[(i + step) % count]) for i in range(count)]


def ring_tables(order):
    count = len(order)
    place = {d: i for i, d in enumerate(order)}
    sources = [[order[(place[d] - s) % count] for s in range(count)] for d in range(count)]
    targets = [[order[(place[d] + s) % count] for s in range(count)] for d in range(count)]
    return np.array(sources, np.int32), np.array(targets, np.int32)


def rotation(count, offset):
    return [(i, (i + offset) % count) for i in range(count)]


def project_kernel(slots, blocks, width, meta, *refs):
    x_refs = refs[:slots]
    table_ref = refs[slots]
    w_refs = refs[slots + 1 : slots + 1 + blocks]
    q_ref, kv_ref, x_buf, w_buf, x_sem, w_sem = refs[slots + 1 + blocks :]
    rows = w_refs[0].shape[1]
    head = w_refs[0].shape[2]
    x_copies = [
        pltpu.make_async_copy(x_refs[s], x_buf.at[s], x_sem.at[s]) for s in range(slots)
    ]
    for copy in x_copies:
        copy.start()
    w_copies = []
    for j in range(blocks):
        first = pl.multiple_of(meta[slots + j] * rows, rows)
        for i in range(3):
            w_copies.append(
                pltpu.make_async_copy(
                    w_refs[j].at[i],
                    w_buf.at[pl.ds(first, rows), pl.ds(i * head, head)],
                    w_sem.at[j, i],
                )
            )
    for copy in w_copies:
        copy.start()
    total = None
    for s in range(slots):
        x_copies[s].wait()
        part = jnp.sum(x_buf[s].astype(jnp.float32), axis=1, keepdims=True)
        total = part if total is None else total + part
    features = slots * width
    average = total / features
    total = None
    for s in range(slots):
        centered = x_buf[s].astype(jnp.float32) - average
        part = jnp.sum(centered * centered, axis=1, keepdims=True)
        total = part if total is None else total + part
    inverse = lax.rsqrt(total / features + epsilon)
    for copy in w_copies:
        copy.wait()
    acc = None
    for s in range(slots):
        normed = (x_buf[s].astype(jnp.float32) - average) * inverse
        modulated = (normed * (1.0 + table_ref[s, 1:2, :]) + table_ref[s, 0:1, :]).astype(
            jnp.bfloat16
        )
        first = pl.multiple_of(meta[s] * width, width)
        part = jnp.dot(
            modulated, w_buf[pl.ds(first, width), :], preferred_element_type=jnp.float32
        )
        acc = part if acc is None else acc + part
    result = acc.astype(jnp.bfloat16)
    q_ref[...] = result[:, :head]
    kv_ref[...] = result[:, head:]


def project(meta, x_slots, table, w_parts):
    slots, blocks = len(x_slots), len(w_parts)
    rows, width = x_slots[0].shape
    _, w_rows, head = w_parts[0].shape
    return pl.pallas_call(
        functools.partial(project_kernel, slots, blocks, width),
        out_shape=(
            jax.ShapeDtypeStruct((rows, head), jnp.bfloat16),
            jax.ShapeDtypeStruct((rows, 2 * head), jnp.bfloat16),
        ),
        in_specs=[SMEM] + [ANY] * slots + [VMEM] + [ANY] * blocks,
        out_specs=(VMEM, VMEM),
        scratch_shapes=[
            pltpu.VMEM((slots, rows, width), jnp.bfloat16),
            pltpu.VMEM((blocks * w_rows, 3 * head), jnp.bfloat16),
            pltpu.SemaphoreType.DMA((slots,)),
            pltpu.SemaphoreType.DMA((blocks, 3)),
        ],
        name="project",
    )(meta, *x_slots, table, *w_parts)


def attend_kernel(q_count, kv_count, factor, live, *refs):
    q_refs = refs[:q_count]
    kv_refs = refs[q_count : q_count + kv_count]
    out_ref = refs[q_count + kv_count]
    first = 0
    for q_ref in q_refs:
        rows, head = q_ref.shape
        queries = q_ref[...]
        scores = [
            lax.dot_general(
                queries,
                kv_ref[:, :head],
                (((1,), (1,)), ((), ())),
                preferred_element_type=jnp.float32,
            )
            * factor
            for kv_ref in kv_refs
        ]
        largest = functools.reduce(
            jnp.maximum, [jnp.max(block, axis=1, keepdims=True) for block in scores]
        )
        totals, weighted = 0.0, 0.0
        for block, kv_ref in zip(scores, kv_refs):
            weights = jnp.exp(block - largest)
            totals = totals + jnp.sum(weights, axis=1, keepdims=True)
            weighted = weighted + jnp.dot(
                weights.astype(jnp.bfloat16),
                kv_ref[:, head:],
                preferred_element_type=jnp.float32,
            )
        attended = weighted / totals
        out_ref[first : first + rows, :] = jnp.where(live[0] > 0, attended, 0.0).astype(
            jnp.bfloat16
        )
        first += rows


def attend(live, q_parts, kv_parts, factor):
    rows = sum(q.shape[0] for q in q_parts)
    return pl.pallas_call(
        functools.partial(attend_kernel, len(q_parts), len(kv_parts), factor),
        out_shape=jax.ShapeDtypeStruct((rows, q_parts[0].shape[1]), jnp.bfloat16),
        in_specs=[SMEM] + [VMEM] * (len(q_parts) + len(kv_parts)),
        out_specs=VMEM,
        name="attend",
    )(live, *q_parts, *kv_parts)


def output_kernel(count, *refs):
    att_refs = refs[:count]
    w_refs = refs[count : 2 * count]
    gate_ref, out_ref = refs[2 * count :]
    acc = None
    for att_ref, w_ref in zip(att_refs, w_refs):
        part = jnp.dot(att_ref[...], w_ref[...], preferred_element_type=jnp.float32)
        acc = part if acc is None else acc + part
    out_ref[...] = (acc * gate_ref[...]).astype(jnp.bfloat16)


def output(att_slots, w_slots, gate):
    count = len(att_slots)
    return pl.pallas_call(
        functools.partial(output_kernel, count),
        out_shape=jax.ShapeDtypeStruct(
            (att_slots[0].shape[0], w_slots[0].shape[1]), jnp.bfloat16
        ),
        in_specs=[VMEM] * (2 * count + 1),
        out_specs=VMEM,
        name="output",
    )(*att_slots, *w_slots, gate)


def body(sizes, tokens, timestep, padded_heads, modulation, qkv_weight, out_weight):
    n_seq, n_tp, n_blk = sizes
    slices = n_seq * n_tp
    seq_at, tp_at, blk_at = (lax.axis_index(a) for a in ("seq", "tp", "blk"))
    own_index = seq_at * n_tp + tp_at
    own_width = tokens.shape[1]
    head_size = out_weight.shape[0]
    order = folded_order(n_seq)
    ring = ring_pairs(order)
    source_table, target_table = ring_tables(order)
    sources = lax.dynamic_index_in_dim(jnp.asarray(source_table), seq_at, 0, keepdims=False)
    targets = lax.dynamic_index_in_dim(jnp.asarray(target_table), seq_at, 0, keepdims=False)

    half = tokens.shape[0] // 2
    current = [tokens[:half], tokens[half:]]
    slots = [[], []]
    for step in range(n_seq):
        if step:
            current = [lax.ppermute(c, "seq", ring) for c in current]
        for chunk in range(2):
            slots[chunk].append(current[chunk])
            for u in range(1, n_tp):
                slots[chunk].append(lax.ppermute(current[chunk], "tp", rotation(n_tp, u)))
    slot_index = jnp.concatenate(
        [sources[:, None] * n_tp + (tp_at - jnp.arange(n_tp, dtype=jnp.int32))[None, :] % n_tp]
    ).reshape(-1)

    w_parts = [qkv_weight] + [
        lax.ppermute(qkv_weight, "blk", rotation(n_blk, j)) for j in range(1, n_blk)
    ]
    blk_index = (blk_at - jnp.arange(n_blk, dtype=jnp.int32)) % n_blk

    ow_parts = [out_weight] + [
        lax.ppermute(out_weight, "blk", rotation(n_blk, j)) for j in range(1, n_blk)
    ]
    own_cols = out_weight.shape[1]
    ow_full = jnp.zeros((head_size, n_blk * own_cols), out_weight.dtype)
    for j in range(n_blk):
        ow_full = lax.dynamic_update_slice(ow_full, ow_parts[j], (0, blk_index[j] * own_cols))
    chip_width = n_tp * own_width
    pieces = []
    for s in range(n_seq):
        piece = lax.dynamic_slice(
            ow_full, (0, targets[s] * chip_width), (head_size, chip_width)
        )
        if s:
            piece = lax.ppermute(piece, "seq", ring_pairs(order, s))
        pieces.append(piece)
    split = [[] for _ in range(n_tp)]
    for u in range(n_tp):
        part = jnp.concatenate(
            [
                lax.dynamic_slice(
                    piece, (0, (tp_at + u) % n_tp * own_width), (head_size, own_width)
                )
                for piece in pieces
            ],
            axis=0,
        )
        if u:
            part = lax.ppermute(part, "tp", rotation(n_tp, u))
        split[u] = part.reshape(n_seq, head_size, own_width)
    ow_slots = [split[u][s] for s in range(n_seq) for u in range(n_tp)]

    table_row = lax.dynamic_index_in_dim(modulation, timestep[0], 0, keepdims=False)
    table = table_row.reshape(3, slices, own_width)
    gate = lax.dynamic_index_in_dim(table[2], own_index, 0, keepdims=True)
    table = jnp.swapaxes(jnp.take(table[:2], slot_index, axis=1), 0, 1)

    meta = jnp.concatenate([slot_index, blk_index]).astype(jnp.int32)
    q_parts, kv_parts = [], []
    for chunk in range(2):
        q, kv = project(meta, slots[chunk], table, w_parts)
        q_parts.append(q)
        kv_parts.append(kv)
        for j in range(1, n_blk):
            kv_parts.append(lax.ppermute(kv, "blk", rotation(n_blk, j)))

    live = (own_index < slices - padded_heads[0]).astype(jnp.int32)[None]
    masked = attend(live, q_parts, kv_parts, 1.0 / math.sqrt(head_size))
    att_slots = []
    current = masked
    for step in range(n_seq):
        if step:
            current = lax.ppermute(current, "seq", ring)
        att_slots.append(current)
        for u in range(1, n_tp):
            att_slots.append(lax.ppermute(current, "tp", rotation(n_tp, u)))
    return output(att_slots, ow_slots, gate)


def solution(mesh):
    sizes = tuple(mesh.shape[a] for a in ("seq", "tp", "blk"))
    return jax.shard_map(
        functools.partial(body, sizes),
        mesh=mesh,
        in_specs=(
            P(("group", "blk"), ("seq", "tp")),
            P("group"),
            P("group"),
            P(),
            P(None, "blk", ("seq", "tp")),
            P(("seq", "tp"), "blk"),
        ),
        out_specs=P(("group", "blk"), ("seq", "tp")),
        check_vma=False,
    )
```

```python
import functools
import math

import jax
import jax.numpy as jnp
from jax import lax
from jax.experimental import pallas as pl
from jax.experimental.pallas import tpu as pltpu
from jax.sharding import PartitionSpec as P

epsilon = 1e-06
ANY = pl.BlockSpec(memory_space=pl.ANY)
VMEM = pl.BlockSpec(memory_space=pltpu.VMEM)
SMEM = pl.BlockSpec(memory_space=pltpu.SMEM)
PARAMS = pltpu.CompilerParams(vmem_limit_bytes=16 << 20)
LANES = 128
f32, bf16 = jnp.float32, jnp.bfloat16


def folded_order(count):
    return list(range(1, count, 2)) + list(range(0, count, 2))[::-1]


def ring_pairs(order, step=1):
    count = len(order)
    return [(order[i], order[(i + step) % count]) for i in range(count)]


def ring_source(count, at, step):
    order = folded_order(count)
    source = 0
    for i, device in enumerate(order):
        source = jnp.where(at == device, order[(i - step) % count], source)
    return source


def rotation(count, offset):
    return [(i, (i + offset) % count) for i in range(count)]


def back(at, offset, count):
    return lax.rem(at + count - offset, count)


def near(x):
    return pltpu.with_memory_space_constraint(x, pltpu.VMEM)


def far(x):
    return pltpu.with_memory_space_constraint(x, pltpu.HBM)


def kernel(body, outs, ins, scratch=()):
    specs = {"near": VMEM, "far": ANY, "smem": SMEM}
    places = {"near": near, "far": far, "smem": lambda x: x}
    return pl.pallas_call(
        body,
        out_shape=tuple(pltpu.VMEM(shape, dtype) for shape, dtype in outs),
        in_specs=[specs[where] for _, where in ins],
        out_specs=tuple(VMEM for _ in outs),
        scratch_shapes=list(scratch),
        compiler_params=PARAMS,
    )(*[places[where](x) for x, where in ins])


def run_copies(copies):
    for copy in copies:
        copy.start()
    for copy in copies:
        copy.wait()


def split_body(x_ref, top_ref, bottom_ref, sem):
    half = top_ref.shape[0]
    run_copies(
        [
            pltpu.make_async_copy(x_ref.at[pl.ds(0, half)], top_ref, sem.at[0]),
            pltpu.make_async_copy(x_ref.at[pl.ds(half, half)], bottom_ref, sem.at[1]),
        ]
    )


def thirds_body(w_ref, relayed_ref, direct_ref, sem):
    run_copies(
        [
            pltpu.make_async_copy(w_ref.at[lax.axis_index("group")], relayed_ref, sem.at[0]),
            pltpu.make_async_copy(w_ref.at[2], direct_ref, sem.at[1]),
        ]
    )


def column_of(sizes, shift, u, width):
    _, n_seq, n_blk, n_tp = sizes
    n_low = n_seq // n_blk
    if shift is None:
        shift = lax.axis_index("group")
    place = lax.rem(lax.rem(lax.axis_index("seq"), n_low) + shift, n_low)
    core = lax.rem(lax.axis_index("tp") + u, n_tp)
    return pl.multiple_of((place * n_tp + core) * width, math.gcd(width, LANES))


def columns_body(sizes, shift, w_ref, *refs):
    *out_refs, sem = refs
    width = out_refs[0].shape[1]
    run_copies(
        [
            pltpu.make_async_copy(
                w_ref.at[:, pl.ds(column_of(sizes, shift, u, width), width)], out_ref, sem.at[u]
            )
            for u, out_ref in enumerate(out_refs)
        ]
    )


def stack_body(*refs):
    *in_refs, out_ref = refs
    rows = in_refs[0].shape[0]
    for i, in_ref in enumerate(in_refs):
        out_ref[i * rows : (i + 1) * rows, :] = in_ref[...]


def merge_body(pieces, table_ref, *refs):
    w_refs = refs[: len(pieces)]
    out_ref, vec_ref, sem = refs[len(pieces) :]
    blk_at, grp_at = lax.axis_index("blk"), lax.axis_index("group")
    copies = []
    for j, (planes, place, column) in enumerate(pieces):
        rows, head = w_refs[j].shape[-2:]
        first = pl.multiple_of(place(blk_at) * rows, rows)
        for i in range(planes):
            source = w_refs[j].at[i] if planes > 1 else w_refs[j]
            at = i * head if planes > 1 else pl.multiple_of(column(grp_at) * head, head)
            copies.append(
                pltpu.make_async_copy(
                    source, out_ref.at[pl.ds(first, rows), pl.ds(at, head)], sem.at[j, i]
                )
            )
    run_copies(copies)
    _, slices, width = table_ref.shape
    total = None
    for f in range(slices):
        shift, scale = table_ref[0, f : f + 1, :], 1.0 + table_ref[1, f : f + 1, :]
        rest = jnp.concatenate([scale, shift], axis=0)
        parts = []
        for _ in range(3):
            part = rest.astype(bf16)
            parts.append(part)
            rest = rest - part.astype(f32)
        vectors = jnp.concatenate(
            [p.astype(f32) for p in parts] + [jnp.zeros((2, width), f32)], axis=0
        ).astype(bf16)
        part = jnp.dot(
            vectors, out_ref[f * width : (f + 1) * width, :], preferred_element_type=f32
        )
        total = part if total is None else total + part
    vec_ref[0:2, :] = total[0:2] + total[2:4] + total[4:6]


def fold(values):
    width = values.shape[1]
    if width % LANES:
        return jnp.sum(values, axis=1, keepdims=True)
    return functools.reduce(
        jnp.add, [values[:, i : i + LANES] for i in range(0, width, LANES)]
    )


def slot_place(sizes, step, u):
    _, n_seq, _, n_tp = sizes
    source = ring_source(n_seq, lax.axis_index("seq"), step)
    return source * n_tp + back(lax.axis_index("tp"), u, n_tp)


def early_body(sizes, slots, table_ref, *refs):
    x_refs = refs[: len(slots)]
    y_ref, mean_ref, square_ref = refs[len(slots) :]
    rows, width = x_refs[0].shape
    tile = 32 if rows % 32 == 0 else rows
    scales = [1.0 + table_ref[1, pl.ds(slot_place(sizes, *slot), 1), :] for slot in slots]

    def step(t, _):
        at = pl.ds(pl.multiple_of(t * tile, tile), tile)
        total = functools.reduce(jnp.add, [fold(x_ref[at, :].astype(f32)) for x_ref in x_refs])
        average = jnp.sum(total, axis=1, keepdims=True) / (len(slots) * width)
        total = None
        for s, x_ref in enumerate(x_refs):
            centred = x_ref[at, :].astype(f32) - average
            y_ref[s, at, :] = (centred * scales[s]).astype(bf16)
            part = fold(centred * centred)
            total = part if total is None else total + part
        mean_ref[at, :] = jnp.broadcast_to(average, (tile, LANES))
        square_ref[at, :] = jnp.broadcast_to(
            jnp.sum(total, axis=1, keepdims=True), (tile, LANES)
        )
        return 0

    lax.fori_loop(0, rows // tile, step, 0)


def project_body(sizes, early, last, table_ref, w_ref, vec_ref, y_ref, mean_ref, square_ref, *refs):
    x_refs = refs[: len(last)]
    q_ref, kv_ref, buf = refs[len(last) :]
    _, width = x_refs[0].shape
    head = q_ref.shape[1]
    features = (len(early) + len(last)) * width
    centre = mean_ref[:, 0:1]
    total, squares = None, None
    for s, x_ref in enumerate(x_refs):
        scale = 1.0 + table_ref[1, pl.ds(slot_place(sizes, *last[s]), 1), :]
        centred = x_ref[...].astype(f32) - centre
        buf[s] = (centred * scale).astype(bf16)
        part, square = fold(centred), fold(centred * centred)
        total = part if total is None else total + part
        squares = square if squares is None else squares + square
    delta = jnp.sum(total, axis=1, keepdims=True) / features
    spread = (square_ref[:, 0:1] + jnp.sum(squares, axis=1, keepdims=True)) / features
    inverse = lax.rsqrt(spread - delta * delta + epsilon)
    acc = None
    for s, slot in enumerate(early + last):
        first = pl.multiple_of(slot_place(sizes, *slot) * width, width)
        values = y_ref[s] if s < len(early) else buf[s - len(early)]
        part = jnp.dot(values, w_ref[pl.ds(first, width), :], preferred_element_type=f32)
        acc = part if acc is None else acc + part
    result = ((acc - delta * vec_ref[0:1, :]) * inverse + vec_ref[1:2, :]).astype(bf16)
    q_ref[...] = result[:, :head]
    kv_ref[...] = result[:, head:]


def attend_body(q_count, kv_count, factor, first, last, live_heads, *refs):
    q_refs = refs[:q_count]
    kv_refs = refs[q_count : q_count + kv_count]
    refs = refs[q_count + kv_count :]
    if not first:
        old_refs, refs = refs[:3], refs[3:]
    row = 0
    for q_ref in q_refs:
        rows, head = q_ref.shape
        at = slice(row, row + rows)
        queries = q_ref[...]
        scores = [
            lax.dot_general(
                queries,
                kv_ref[:, :head],
                (((1,), (1,)), ((), ())),
                preferred_element_type=f32,
            )
            * factor
            for kv_ref in kv_refs
        ]
        largest = jnp.max(functools.reduce(jnp.maximum, scores), axis=1, keepdims=True)
        if not first:
            old = old_refs[0][at, 0:1]
            largest = jnp.maximum(largest, old)
            rescale = jnp.exp(old - largest)
        total, weighted = None, None
        for block, kv_ref in zip(scores, kv_refs):
            weights = jnp.exp(block - largest)
            part = jnp.dot(
                weights.astype(bf16), kv_ref[:, head:], preferred_element_type=f32
            )
            weighted = part if weighted is None else weighted + part
            total = weights if total is None else total + weights
        total = jnp.sum(total, axis=1, keepdims=True)
        if not first:
            total = total + old_refs[1][at, 0:1] * rescale
            weighted = weighted + old_refs[2][at, :] * rescale
        if last:
            live = live_heads[0] > 0
            refs[0][at, :] = jnp.where(live, weighted / total, 0.0).astype(bf16)
        else:
            refs[0][at, :] = jnp.broadcast_to(largest, (rows, LANES))
            refs[1][at, :] = jnp.broadcast_to(total, (rows, LANES))
            refs[2][at, :] = weighted
        row += rows


def output_early_body(sizes, slots, last_step, sources, *refs):
    n_tp = sizes[3]
    att_refs = refs[: len(slots)]
    w_refs = refs[len(slots) : len(slots) + len(sources)]
    acc_ref, rest_ref, buf = refs[len(slots) + len(sources) :]
    for w_ref, source in zip(w_refs, sources):
        buf[source()] = w_ref[...]
    seq_at = lax.axis_index("seq")
    acc = None
    for i in range(0, len(slots), n_tp):
        values = jnp.concatenate([r[...] for r in att_refs[i : i + n_tp]], axis=1)
        weight = buf[ring_source(sizes[1], seq_at, slots[i][0])]
        part = jnp.dot(values, weight, preferred_element_type=f32)
        acc = part if acc is None else acc + part
    acc_ref[...] = acc
    rest_ref[...] = buf[ring_source(sizes[1], seq_at, last_step)]


def output_body(sizes, table_ref, acc_ref, w_ref, *refs):
    *att_refs, out_ref = refs
    values = jnp.concatenate([r[...] for r in att_refs], axis=1)
    summed = acc_ref[...] + jnp.dot(values, w_ref[...], preferred_element_type=f32)
    own = lax.axis_index("seq") * sizes[3] + lax.axis_index("tp")
    out_ref[...] = (summed * table_ref[2, pl.ds(own, 1), :]).astype(bf16)


def shares_weights(sizes):
    n_grp, _, n_blk, _ = sizes
    return n_grp == 2 and n_blk == 2


def shares_columns(sizes):
    n_grp, n_seq, n_blk, _ = sizes
    return n_grp == n_seq // n_blk


def body(sizes, *arrays):
    return block(sizes, *arrays)


def block(sizes, tokens, timestep, padded_heads, modulation, qkv_weight, out_weight):
    n_grp, n_seq, n_blk, n_tp = sizes
    slices = n_seq * n_tp
    own_width = tokens.shape[1]
    half = tokens.shape[0] // 2
    head = out_weight.shape[0]
    order = folded_order(n_seq)
    forward, backward = ring_pairs(order), ring_pairs(order, -1)
    DMA = pltpu.SemaphoreType.DMA

    current = list(
        kernel(split_body, [((half, own_width), bf16)] * 2, [(tokens, "far")], [DMA((2,))])
    )
    slots = [{}, {}]
    for step in range(n_seq):
        for chunk in range(2):
            if step:
                current[chunk] = lax.ppermute(current[chunk], "seq", forward)
            slots[chunk][step, 0] = current[chunk]
            for u in range(1, n_tp):
                slots[chunk][step, u] = lax.ppermute(current[chunk], "tp", rotation(n_tp, u))

    table = lax.dynamic_index_in_dim(modulation, timestep[0], 0, keepdims=False)
    table = table.reshape(3, slices, own_width)

    parts, pieces = [(qkv_weight, "far")], [(3, lambda b: b, None)]
    if shares_weights(sizes):
        relayed, direct = kernel(
            thirds_body, [(qkv_weight.shape[1:], bf16)] * 2, [(qkv_weight, "far")], [DMA((2,))]
        )
        first = lax.ppermute(relayed, "blk", rotation(2, 1))
        second = lax.ppermute(direct, "blk", rotation(2, 1))
        third = lax.ppermute(first, "group", rotation(2, 1))
        parts += [(first, "near"), (second, "near"), (third, "near")]
        pieces += [
            (1, lambda b: 1 - b, lambda g: g),
            (1, lambda b: 1 - b, lambda g: 2),
            (1, lambda b: 1 - b, lambda g: 1 - g),
        ]
    else:
        for j in range(1, n_blk):
            parts.append((lax.ppermute(qkv_weight, "blk", rotation(n_blk, j)), "near"))
            pieces.append((3, lambda b, j=j: back(b, j, n_blk), None))
    weight, vectors = kernel(
        functools.partial(merge_body, pieces),
        [((slices * own_width, 3 * head), bf16), ((8, 3 * head), f32)],
        [(table, "near")] + parts,
        [DMA((len(pieces), 3))],
    )

    n_low = n_seq // n_blk
    shared = shares_columns(sizes)
    o_parts, o_sources = [], []

    def source_of(k3, shift):
        def source():
            low = lax.rem(lax.axis_index("seq"), n_low)
            s = back(lax.axis_index("group"), -shift, n_grp) if shared else shift
            return back(lax.axis_index("blk"), k3, n_blk) * n_low + lax.rem(low - s + n_low, n_low)

        return source

    for k1 in range(1 if shared else n_low):
        received = list(
            kernel(
                functools.partial(columns_body, sizes, None if shared else k1),
                [((head, own_width), bf16)] * n_tp,
                [(out_weight, "far")],
                [DMA((n_tp,))],
            )
            if own_width % LANES == 0
            else [
                lax.dynamic_slice(
                    out_weight,
                    (0, column_of(sizes, None if shared else k1, u, own_width)),
                    (head, own_width),
                )
                for u in range(n_tp)
            ]
        )
        for u in range(1, n_tp):
            received[u] = lax.ppermute(received[u], "tp", rotation(n_tp, u))
        (rows,) = kernel(
            stack_body, [((n_tp * head, own_width), bf16)], [(x, "near") for x in received]
        )
        for k3 in range(1 if shared else n_blk):
            pairs = []
            for g in range(n_grp):
                for z in range(n_seq):
                    for b in range(n_blk):
                        l2 = (z % n_low + (g if shared else k1)) % n_low
                        target = (g * n_seq + b * n_low + l2) * n_blk + (z // n_low + k3) % n_blk
                        pairs.append(((g * n_seq + z) * n_blk + b, target))
            arrived = lax.ppermute(rows, ("group", "seq", "blk"), pairs)
            o_parts.append(arrived)
            o_sources.append(source_of(k3, 0 if shared else k1))
        if shared:
            for g in range(n_grp):
                for j in range(n_blk):
                    if g or j:
                        swap = [
                            (p * n_blk + b, (p + g) % n_grp * n_blk + (b + j) % n_blk)
                            for p in range(n_grp)
                            for b in range(n_blk)
                        ]
                        o_parts.append(lax.ppermute(arrived, ("group", "blk"), swap))
                        o_sources.append(source_of(j, -g))

    early = [(s, u) for s in range(n_seq - 1) for u in range(n_tp)]
    last = [(n_seq - 1, u) for u in range(n_tp)]
    starts = [
        kernel(
            functools.partial(early_body, sizes, early),
            [
                ((len(early), half, own_width), bf16),
                ((half, LANES), f32),
                ((half, LANES), f32),
            ],
            [(table, "near")] + [(slots[chunk][slot], "near") for slot in early],
        )
        for chunk in range(2)
    ]
    q_parts, kv_own, kv_rest = [], [], []
    for chunk in range(2):
        q, kv = kernel(
            functools.partial(project_body, sizes, early, last),
            [((half, head), bf16), ((half, 2 * head), bf16)],
            [(x, "near") for x in (table, weight, vectors, *starts[chunk])]
            + [(slots[chunk][slot], "near") for slot in last],
            [pltpu.VMEM((len(last), half, own_width), bf16)],
        )
        q_parts.append(q)
        kv_own.append(kv)
        for j in range(1, n_blk):
            kv_rest.append(lax.ppermute(kv, "blk", rotation(n_blk, j)))

    own_index = lax.axis_index("seq") * n_tp + lax.axis_index("tp")
    live = (own_index < slices - padded_heads).astype(jnp.int32)
    factor = 1.0 / math.sqrt(head)
    state = kernel(
        functools.partial(attend_body, 2, len(kv_own), factor, True, False),
        [((2 * half, LANES), f32), ((2 * half, LANES), f32), ((2 * half, head), f32)],
        [(live, "smem")] + [(x, "near") for x in q_parts + kv_own],
    )
    (masked,) = kernel(
        functools.partial(attend_body, 2, len(kv_rest), factor, False, True),
        [((2 * half, head), bf16)],
        [(live, "smem")] + [(x, "near") for x in (*q_parts, *kv_rest, *state)],
    )

    att = {(0, 0): masked}
    up, down = masked, masked
    last_step = n_seq // 2
    for step in range(1, last_step + 1):
        up = att[step, 0] = lax.ppermute(up, "seq", forward)
        if n_seq - step > step:
            down = att[n_seq - step, 0] = lax.ppermute(down, "seq", backward)
    for step in range(n_seq):
        for u in range(1, n_tp):
            att[step, u] = lax.ppermute(att[step, 0], "tp", rotation(n_tp, u))
    first_slots = [(s, u) for s in range(n_seq) if s != last_step for u in range(n_tp)]
    acc, rest = kernel(
        functools.partial(output_early_body, sizes, first_slots, last_step, o_sources),
        [((2 * half, own_width), f32), ((n_tp * head, own_width), bf16)],
        [(att[slot], "near") for slot in first_slots] + [(x, "near") for x in o_parts],
        [pltpu.VMEM((n_seq, n_tp * head, own_width), bf16)],
    )
    return pl.pallas_call(
        functools.partial(output_body, sizes),
        out_shape=jax.ShapeDtypeStruct((2 * half, own_width), bf16),
        in_specs=[VMEM] * (3 + n_tp),
        out_specs=VMEM,
        compiler_params=PARAMS,
        name="output",
    )(near(table), near(acc), near(rest), *[near(att[last_step, u]) for u in range(n_tp)])


def solution(mesh):
    sizes = tuple(mesh.shape[a] for a in ("group", "seq", "blk", "tp"))
    return jax.shard_map(
        functools.partial(body, sizes),
        mesh=mesh,
        in_specs=(
            P(("group", "blk"), ("seq", "tp")),
            P("group"),
            P("group"),
            P(),
            P(None, "blk", ("seq", "tp")),
            P(("seq", "tp"), "blk"),
        ),
        out_specs=P(("group", "blk"), ("seq", "tp")),
        check_vma=False,
    )
```

```python
import functools
import math

import jax
import jax.numpy as jnp
from jax import lax
from jax.experimental import pallas as pl
from jax.experimental.pallas import tpu as pltpu
from jax.sharding import PartitionSpec as P

epsilon = 1e-06
ANY = pl.BlockSpec(memory_space=pl.ANY)
VMEM = pl.BlockSpec(memory_space=pltpu.VMEM)
SMEM = pl.BlockSpec(memory_space=pltpu.SMEM)
PARAMS = pltpu.CompilerParams(vmem_limit_bytes=16 << 20)
LANES = 128
f32, bf16 = jnp.float32, jnp.bfloat16


def folded_order(count):
    return list(range(1, count, 2)) + list(range(0, count, 2))[::-1]


def ring_pairs(order, step=1):
    count = len(order)
    return [(order[i], order[(i + step) % count]) for i in range(count)]


def ring_source(count, at, step):
    order = folded_order(count)
    source = 0
    for i, device in enumerate(order):
        source = jnp.where(at == device, order[(i - step) % count], source)
    return source


def rotation(count, offset):
    return [(i, (i + offset) % count) for i in range(count)]


def back(at, offset, count):
    return lax.rem(at + count - offset, count)


def near(x):
    return pltpu.with_memory_space_constraint(x, pltpu.VMEM)


def far(x):
    return pltpu.with_memory_space_constraint(x, pltpu.HBM)


def kernel(body, outs, ins, scratch=()):
    specs = {"near": VMEM, "far": ANY, "smem": SMEM}
    places = {"near": near, "far": far, "smem": lambda x: x}
    return pl.pallas_call(
        body,
        out_shape=tuple(pltpu.VMEM(shape, dtype) for shape, dtype in outs),
        in_specs=[specs[where] for _, where in ins],
        out_specs=tuple(VMEM for _ in outs),
        scratch_shapes=list(scratch),
        compiler_params=PARAMS,
    )(*[places[where](x) for x, where in ins])


def run_copies(copies):
    for copy in copies:
        copy.start()
    for copy in copies:
        copy.wait()


def split_body(shared, x_ref, w_ref, top_ref, bottom_ref, *refs):
    half = top_ref.shape[0]
    sem = refs[-1]
    copies = [
        pltpu.make_async_copy(x_ref.at[pl.ds(0, half)], top_ref, sem.at[0]),
        pltpu.make_async_copy(x_ref.at[pl.ds(half, half)], bottom_ref, sem.at[1]),
    ]
    if shared:
        plane = lax.axis_index("group")
        copies += [
            pltpu.make_async_copy(w_ref.at[plane], refs[0], sem.at[2]),
            pltpu.make_async_copy(w_ref.at[2], refs[1], sem.at[3]),
        ]
    run_copies(copies)


def table_body(at, m_ref, out_ref):
    _, slices, width = out_ref.shape
    for i in range(3):
        row = m_ref[i, pl.ds(at[0], 1), :]
        for f in range(slices):
            out_ref[i, f : f + 1, :] = row[:, f * width : (f + 1) * width]


def column_of(sizes, shift, u, width):
    _, n_seq, n_blk, n_tp = sizes
    n_low = n_seq // n_blk
    if shift is None:
        shift = lax.axis_index("group")
    place = lax.rem(lax.rem(lax.axis_index("seq"), n_low) + shift, n_low)
    core = lax.rem(lax.axis_index("tp") + u, n_tp)
    return pl.multiple_of((place * n_tp + core) * width, math.gcd(width, LANES))


def columns_body(sizes, shift, w_ref, *refs):
    *out_refs, sem = refs
    width = out_refs[0].shape[1]
    run_copies(
        [
            pltpu.make_async_copy(
                w_ref.at[:, pl.ds(column_of(sizes, shift, u, width), width)], out_ref, sem.at[u]
            )
            for u, out_ref in enumerate(out_refs)
        ]
    )


def stack_body(*refs):
    *in_refs, out_ref = refs
    rows = in_refs[0].shape[0]
    for i, in_ref in enumerate(in_refs):
        out_ref[i * rows : (i + 1) * rows, :] = in_ref[...]


def merge_body(pieces, table_ref, *refs):
    w_refs = refs[: len(pieces)]
    out_ref, vec_ref, sem = refs[len(pieces) :]
    blk_at, grp_at = lax.axis_index("blk"), lax.axis_index("group")
    copies = []
    for j, (planes, place, column) in enumerate(pieces):
        rows, head = w_refs[j].shape[-2:]
        first = pl.multiple_of(place(blk_at) * rows, rows)
        for i in range(planes):
            source = w_refs[j].at[i] if planes > 1 else w_refs[j]
            at = i * head if planes > 1 else pl.multiple_of(column(grp_at) * head, head)
            copies.append(
                pltpu.make_async_copy(
                    source, out_ref.at[pl.ds(first, rows), pl.ds(at, head)], sem.at[j, i]
                )
            )
    run_copies(copies)
    _, slices, width = table_ref.shape
    total = None
    for f in range(slices):
        shift, scale = table_ref[0, f : f + 1, :], 1.0 + table_ref[1, f : f + 1, :]
        rest = jnp.concatenate([scale, shift], axis=0)
        parts = []
        for _ in range(3):
            part = rest.astype(bf16)
            parts.append(part)
            rest = rest - part.astype(f32)
        vectors = jnp.concatenate(
            [p.astype(f32) for p in parts] + [jnp.zeros((2, width), f32)], axis=0
        ).astype(bf16)
        part = jnp.dot(
            vectors, out_ref[f * width : (f + 1) * width, :], preferred_element_type=f32
        )
        total = part if total is None else total + part
    vec_ref[0:2, :] = total[0:2] + total[2:4] + total[4:6]


def fold(values):
    width = values.shape[1]
    if width % LANES:
        return jnp.sum(values, axis=1, keepdims=True)
    return functools.reduce(
        jnp.add, [values[:, i : i + LANES] for i in range(0, width, LANES)]
    )


def slot_place(sizes, step, u):
    _, n_seq, _, n_tp = sizes
    source = ring_source(n_seq, lax.axis_index("seq"), step)
    return source * n_tp + back(lax.axis_index("tp"), u, n_tp)


def early_body(sizes, slots, table_ref, *refs):
    x_refs = refs[: len(slots)]
    y_ref, mean_ref, square_ref = refs[len(slots) :]
    rows, width = x_refs[0].shape
    tile = rows
    scales = [1.0 + table_ref[1, pl.ds(slot_place(sizes, *slot), 1), :] for slot in slots]

    def step(t, _):
        at = pl.ds(pl.multiple_of(t * tile, tile), tile)
        total = functools.reduce(jnp.add, [fold(x_ref[at, :].astype(f32)) for x_ref in x_refs])
        average = jnp.sum(total, axis=1, keepdims=True) / (len(slots) * width)
        total = None
        for s, x_ref in enumerate(x_refs):
            centred = x_ref[at, :].astype(f32) - average
            y_ref[s, at, :] = (centred * scales[s]).astype(bf16)
            part = fold(centred * centred)
            total = part if total is None else total + part
        mean_ref[at, :] = jnp.broadcast_to(average, (tile, LANES))
        square_ref[at, :] = jnp.broadcast_to(
            jnp.sum(total, axis=1, keepdims=True), (tile, LANES)
        )
        return 0

    lax.fori_loop(0, rows // tile, step, 0)


def project_body(sizes, early, last, table_ref, w_ref, vec_ref, y_ref, mean_ref, square_ref, *refs):
    x_refs = refs[: len(last)]
    q_ref, kv_ref, buf = refs[len(last) :]
    _, width = x_refs[0].shape
    head = q_ref.shape[1]
    features = (len(early) + len(last)) * width
    centre = mean_ref[:, 0:1]
    total, squares = None, None
    for s, x_ref in enumerate(x_refs):
        scale = 1.0 + table_ref[1, pl.ds(slot_place(sizes, *last[s]), 1), :]
        centred = x_ref[...].astype(f32) - centre
        buf[s] = (centred * scale).astype(bf16)
        part, square = fold(centred), fold(centred * centred)
        total = part if total is None else total + part
        squares = square if squares is None else squares + square
    delta = jnp.sum(total, axis=1, keepdims=True) / features
    spread = (square_ref[:, 0:1] + jnp.sum(squares, axis=1, keepdims=True)) / features
    inverse = lax.rsqrt(spread - delta * delta + epsilon)
    acc = None
    for s, slot in enumerate(early + last):
        first = pl.multiple_of(slot_place(sizes, *slot) * width, width)
        values = y_ref[s] if s < len(early) else buf[s - len(early)]
        part = jnp.dot(values, w_ref[pl.ds(first, width), :], preferred_element_type=f32)
        acc = part if acc is None else acc + part
    result = ((acc - delta * vec_ref[0:1, :]) * inverse + vec_ref[1:2, :]).astype(bf16)
    q_ref[...] = result[:, :head]
    kv_ref[...] = result[:, head:]


def attend_body(sizes, q_count, kv_count, factor, first, last, padded, *refs):
    q_refs = refs[:q_count]
    kv_refs = refs[q_count : q_count + kv_count]
    refs = refs[q_count + kv_count :]
    if not first:
        old_refs, refs = refs[:3], refs[3:]
    row = 0
    for q_ref in q_refs:
        rows, head = q_ref.shape
        at = slice(row, row + rows)
        queries = q_ref[...]
        scores = [
            lax.dot_general(
                queries,
                kv_ref[:, :head],
                (((1,), (1,)), ((), ())),
                preferred_element_type=f32,
            )
            * factor
            for kv_ref in kv_refs
        ]
        largest = jnp.max(functools.reduce(jnp.maximum, scores), axis=1, keepdims=True)
        if not first:
            old = old_refs[0][at, 0:1]
            largest = jnp.maximum(largest, old)
            rescale = jnp.exp(old - largest)
        total, weighted = None, None
        for block, kv_ref in zip(scores, kv_refs):
            weights = jnp.exp(block - largest)
            part = jnp.dot(
                weights.astype(bf16), kv_ref[:, head:], preferred_element_type=f32
            )
            weighted = part if weighted is None else weighted + part
            total = weights if total is None else total + weights
        total = jnp.sum(total, axis=1, keepdims=True)
        if not first:
            total = total + old_refs[1][at, 0:1] * rescale
            weighted = weighted + old_refs[2][at, :] * rescale
        if last:
            own = lax.axis_index("seq") * sizes[3] + lax.axis_index("tp")
            live = own < sizes[1] * sizes[3] - padded[0]
            refs[0][at, :] = jnp.where(live, weighted / total, 0.0).astype(bf16)
        else:
            refs[0][at, :] = jnp.broadcast_to(largest, (rows, LANES))
            refs[1][at, :] = jnp.broadcast_to(total, (rows, LANES))
            refs[2][at, :] = weighted
        row += rows


def output_early_body(sizes, slots, last_step, sources, *refs):
    n_tp = sizes[3]
    att_refs = refs[: len(slots)]
    w_refs = refs[len(slots) : len(slots) + len(sources)]
    acc_ref, rest_ref, buf = refs[len(slots) + len(sources) :]
    for w_ref, source in zip(w_refs, sources):
        buf[source()] = w_ref[...]
    seq_at = lax.axis_index("seq")
    acc = None
    for i in range(0, len(slots), n_tp):
        values = jnp.concatenate([r[...] for r in att_refs[i : i + n_tp]], axis=1)
        weight = buf[ring_source(sizes[1], seq_at, slots[i][0])]
        part = jnp.dot(values, weight, preferred_element_type=f32)
        acc = part if acc is None else acc + part
    acc_ref[...] = acc
    rest_ref[...] = buf[ring_source(sizes[1], seq_at, last_step)]


def output_body(sizes, table_ref, acc_ref, w_ref, *refs):
    *att_refs, out_ref = refs
    values = jnp.concatenate([r[...] for r in att_refs], axis=1)
    summed = acc_ref[...] + jnp.dot(values, w_ref[...], preferred_element_type=f32)
    own = lax.axis_index("seq") * sizes[3] + lax.axis_index("tp")
    out_ref[...] = (summed * table_ref[2, pl.ds(own, 1), :]).astype(bf16)


def shares_weights(sizes):
    n_grp, _, n_blk, _ = sizes
    return n_grp == 2 and n_blk == 2


def shares_columns(sizes):
    n_grp, n_seq, n_blk, _ = sizes
    return n_grp == n_seq // n_blk


def body(sizes, *arrays):
    return block(sizes, *arrays)


def block(sizes, tokens, timestep, padded_heads, modulation, qkv_weight, out_weight):
    n_grp, n_seq, n_blk, n_tp = sizes
    slices = n_seq * n_tp
    own_width = tokens.shape[1]
    half = tokens.shape[0] // 2
    head = out_weight.shape[0]
    order = folded_order(n_seq)
    forward, backward = ring_pairs(order), ring_pairs(order, -1)
    DMA = pltpu.SemaphoreType.DMA

    by_two = shares_weights(sizes)
    cut = kernel(
        functools.partial(split_body, by_two),
        [((half, own_width), bf16)] * 2 + [(qkv_weight.shape[1:], bf16)] * (2 if by_two else 0),
        [(tokens, "far"), (qkv_weight, "far")],
        [DMA((4,))],
    )
    current = list(cut[:2])
    slots = [{}, {}]
    for step in range(n_seq):
        for chunk in range(2):
            if step:
                current[chunk] = lax.ppermute(current[chunk], "seq", forward)
            slots[chunk][step, 0] = current[chunk]
            for u in range(1, n_tp):
                slots[chunk][step, u] = lax.ppermute(current[chunk], "tp", rotation(n_tp, u))

    (table,) = kernel(
        table_body,
        [((3, slices, own_width), f32)],
        [(timestep, "smem"), (jnp.swapaxes(modulation, 0, 1), "near")],
    )

    parts, pieces = [(qkv_weight, "far")], [(3, lambda b: b, None)]
    if by_two:
        relayed, direct = cut[2:]
        first = lax.ppermute(relayed, "blk", rotation(2, 1))
        second = lax.ppermute(direct, "blk", rotation(2, 1))
        third = lax.ppermute(first, "group", rotation(2, 1))
        parts += [(first, "near"), (second, "near"), (third, "near")]
        pieces += [
            (1, lambda b: 1 - b, lambda g: g),
            (1, lambda b: 1 - b, lambda g: 2),
            (1, lambda b: 1 - b, lambda g: 1 - g),
        ]
    else:
        for j in range(1, n_blk):
            parts.append((lax.ppermute(qkv_weight, "blk", rotation(n_blk, j)), "near"))
            pieces.append((3, lambda b, j=j: back(b, j, n_blk), None))
    weight, vectors = kernel(
        functools.partial(merge_body, pieces),
        [((slices * own_width, 3 * head), bf16), ((8, 3 * head), f32)],
        [(table, "near")] + parts,
        [DMA((len(pieces), 3))],
    )

    n_low = n_seq // n_blk
    shared = shares_columns(sizes)
    o_parts, o_sources = [], []

    def source_of(k3, shift):
        def source():
            low = lax.rem(lax.axis_index("seq"), n_low)
            s = back(lax.axis_index("group"), -shift, n_grp) if shared else shift
            return back(lax.axis_index("blk"), k3, n_blk) * n_low + lax.rem(low - s + n_low, n_low)

        return source

    for k1 in range(1 if shared else n_low):
        received = list(
            kernel(
                functools.partial(columns_body, sizes, None if shared else k1),
                [((head, own_width), bf16)] * n_tp,
                [(out_weight, "far")],
                [DMA((n_tp,))],
            )
            if own_width % LANES == 0
            else [
                lax.dynamic_slice(
                    out_weight,
                    (0, column_of(sizes, None if shared else k1, u, own_width)),
                    (head, own_width),
                )
                for u in range(n_tp)
            ]
        )
        for u in range(1, n_tp):
            received[u] = lax.ppermute(received[u], "tp", rotation(n_tp, u))
        (rows,) = kernel(
            stack_body, [((n_tp * head, own_width), bf16)], [(x, "near") for x in received]
        )
        for k3 in range(1 if shared else n_blk):
            pairs = []
            for g in range(n_grp):
                for z in range(n_seq):
                    for b in range(n_blk):
                        l2 = (z % n_low + (g if shared else k1)) % n_low
                        target = (g * n_seq + b * n_low + l2) * n_blk + (z // n_low + k3) % n_blk
                        pairs.append(((g * n_seq + z) * n_blk + b, target))
            arrived = lax.ppermute(rows, ("group", "seq", "blk"), pairs)
            o_parts.append(arrived)
            o_sources.append(source_of(k3, 0 if shared else k1))
        if shared:
            for g in range(n_grp):
                for j in range(n_blk):
                    if g or j:
                        swap = [
                            (p * n_blk + b, (p + g) % n_grp * n_blk + (b + j) % n_blk)
                            for p in range(n_grp)
                            for b in range(n_blk)
                        ]
                        o_parts.append(lax.ppermute(arrived, ("group", "blk"), swap))
                        o_sources.append(source_of(j, -g))

    early = [(s, u) for s in range(n_seq - 1) for u in range(n_tp)]
    last = [(n_seq - 1, u) for u in range(n_tp)]
    starts = [
        kernel(
            functools.partial(early_body, sizes, early),
            [
                ((len(early), half, own_width), bf16),
                ((half, LANES), f32),
                ((half, LANES), f32),
            ],
            [(table, "near")] + [(slots[chunk][slot], "near") for slot in early],
        )
        for chunk in range(2)
    ]
    q_parts, kv_own, kv_rest = [], [], []
    for chunk in range(2):
        q, kv = kernel(
            functools.partial(project_body, sizes, early, last),
            [((half, head), bf16), ((half, 2 * head), bf16)],
            [(x, "near") for x in (table, weight, vectors, *starts[chunk])]
            + [(slots[chunk][slot], "near") for slot in last],
            [pltpu.VMEM((len(last), half, own_width), bf16)],
        )
        q_parts.append(q)
        kv_own.append(kv)
        for j in range(1, n_blk):
            kv_rest.append(lax.ppermute(kv, "blk", rotation(n_blk, j)))

    factor = 1.0 / math.sqrt(head)
    state = kernel(
        functools.partial(attend_body, sizes, 2, len(kv_own), factor, True, False),
        [((2 * half, LANES), f32), ((2 * half, LANES), f32), ((2 * half, head), f32)],
        [(padded_heads, "smem")] + [(x, "near") for x in q_parts + kv_own],
    )
    (masked,) = kernel(
        functools.partial(attend_body, sizes, 2, len(kv_rest), factor, False, True),
        [((2 * half, head), bf16)],
        [(padded_heads, "smem")] + [(x, "near") for x in (*q_parts, *kv_rest, *state)],
    )

    att = {(0, 0): masked}
    up, down = masked, masked
    last_step = n_seq // 2
    for step in range(1, last_step + 1):
        up = att[step, 0] = lax.ppermute(up, "seq", forward)
        if n_seq - step > step:
            down = att[n_seq - step, 0] = lax.ppermute(down, "seq", backward)
    for step in range(n_seq):
        for u in range(1, n_tp):
            att[step, u] = lax.ppermute(att[step, 0], "tp", rotation(n_tp, u))
    first_slots = [(s, u) for s in range(n_seq) if s != last_step for u in range(n_tp)]
    acc, rest = kernel(
        functools.partial(output_early_body, sizes, first_slots, last_step, o_sources),
        [((2 * half, own_width), f32), ((n_tp * head, own_width), bf16)],
        [(att[slot], "near") for slot in first_slots] + [(x, "near") for x in o_parts],
        [pltpu.VMEM((n_seq, n_tp * head, own_width), bf16)],
    )
    return pl.pallas_call(
        functools.partial(output_body, sizes),
        out_shape=jax.ShapeDtypeStruct((2 * half, own_width), bf16),
        in_specs=[VMEM] * (3 + n_tp),
        out_specs=VMEM,
        compiler_params=PARAMS,
        name="output",
    )(near(table), near(acc), near(rest), *[near(att[last_step, u]) for u in range(n_tp)])


def solution(mesh):
    sizes = tuple(mesh.shape[a] for a in ("group", "seq", "blk", "tp"))
    return jax.shard_map(
        functools.partial(body, sizes),
        mesh=mesh,
        in_specs=(
            P(("group", "blk"), ("seq", "tp")),
            P("group"),
            P("group"),
            P(),
            P(None, "blk", ("seq", "tp")),
            P(("seq", "tp"), "blk"),
        ),
        out_specs=P(("group", "blk"), ("seq", "tp")),
        check_vma=False,
    )
```

```python
import functools
import math

import jax
import jax.numpy as jnp
from jax import lax
from jax.experimental import pallas as pl
from jax.experimental.pallas import tpu as pltpu
from jax.sharding import PartitionSpec as P

epsilon = 1e-06
ANY = pl.BlockSpec(memory_space=pl.ANY)
VMEM = pl.BlockSpec(memory_space=pltpu.VMEM)
SMEM = pl.BlockSpec(memory_space=pltpu.SMEM)
PARAMS = pltpu.CompilerParams(vmem_limit_bytes=16 << 20)
LANES = 128
f32, bf16 = jnp.float32, jnp.bfloat16


def folded_order(count):
    return list(range(1, count, 2)) + list(range(0, count, 2))[::-1]


def ring_pairs(order, step=1):
    count = len(order)
    return [(order[i], order[(i + step) % count]) for i in range(count)]


def ring_source(count, at, step):
    order = folded_order(count)
    source = 0
    for i, device in enumerate(order):
        source = jnp.where(at == device, order[(i - step) % count], source)
    return source


def rotation(count, offset):
    return [(i, (i + offset) % count) for i in range(count)]


def back(at, offset, count):
    return lax.rem(at + count - offset, count)


def near(x):
    return pltpu.with_memory_space_constraint(x, pltpu.VMEM)


def far(x):
    return pltpu.with_memory_space_constraint(x, pltpu.HBM)


def kernel(body, outs, ins, scratch=()):
    specs = {"near": VMEM, "far": ANY, "smem": SMEM}
    places = {"near": near, "far": far, "smem": lambda x: x}
    return pl.pallas_call(
        body,
        out_shape=tuple(pltpu.VMEM(shape, dtype) for shape, dtype in outs),
        in_specs=[specs[where] for _, where in ins],
        out_specs=tuple(VMEM for _ in outs),
        scratch_shapes=list(scratch),
        compiler_params=PARAMS,
    )(*[places[where](x) for x, where in ins])


def run_copies(copies):
    for copy in copies:
        copy.start()
    for copy in copies:
        copy.wait()


def split_body(shared, x_ref, w_ref, top_ref, bottom_ref, *refs):
    half = top_ref.shape[0]
    sem = refs[-1]
    copies = [
        pltpu.make_async_copy(x_ref.at[pl.ds(0, half)], top_ref, sem.at[0]),
        pltpu.make_async_copy(x_ref.at[pl.ds(half, half)], bottom_ref, sem.at[1]),
    ]
    if shared:
        plane = lax.axis_index("group")
        copies += [
            pltpu.make_async_copy(w_ref.at[plane], refs[0], sem.at[2]),
            pltpu.make_async_copy(w_ref.at[2], refs[1], sem.at[3]),
        ]
    run_copies(copies)


def table_body(at, m_ref, out_ref):
    _, slices, width = out_ref.shape
    for i in range(3):
        row = m_ref[i, pl.ds(at[0], 1), :]
        for f in range(slices):
            out_ref[i, f : f + 1, :] = row[:, f * width : (f + 1) * width]


def column_of(sizes, shift, u, width):
    _, n_seq, n_blk, n_tp = sizes
    n_low = n_seq // n_blk
    if shift is None:
        shift = lax.axis_index("group")
    place = lax.rem(lax.rem(lax.axis_index("seq"), n_low) + shift, n_low)
    core = lax.rem(lax.axis_index("tp") + u, n_tp)
    return pl.multiple_of((place * n_tp + core) * width, math.gcd(width, LANES))


def columns_body(sizes, shift, w_ref, *refs):
    *out_refs, sem = refs
    width = out_refs[0].shape[1]
    run_copies(
        [
            pltpu.make_async_copy(
                w_ref.at[:, pl.ds(column_of(sizes, shift, u, width), width)], out_ref, sem.at[u]
            )
            for u, out_ref in enumerate(out_refs)
        ]
    )


def stack_body(*refs):
    *in_refs, out_ref = refs
    rows = in_refs[0].shape[0]
    for i, in_ref in enumerate(in_refs):
        out_ref[i * rows : (i + 1) * rows, :] = in_ref[...]


def merge_body(pieces, table_ref, *refs):
    w_refs = refs[: len(pieces)]
    out_ref, vec_ref, sem = refs[len(pieces) :]
    blk_at, grp_at = lax.axis_index("blk"), lax.axis_index("group")
    copies = []
    for j, (planes, place, column) in enumerate(pieces):
        rows, head = w_refs[j].shape[-2:]
        first = pl.multiple_of(place(blk_at) * rows, rows)
        for i in range(planes):
            source = w_refs[j].at[i] if planes > 1 else w_refs[j]
            at = i * head if planes > 1 else pl.multiple_of(column(grp_at) * head, head)
            copies.append(
                pltpu.make_async_copy(
                    source, out_ref.at[pl.ds(first, rows), pl.ds(at, head)], sem.at[j, i]
                )
            )
    run_copies(copies)
    _, slices, width = table_ref.shape
    total = None
    for f in range(slices):
        shift, scale = table_ref[0, f : f + 1, :], 1.0 + table_ref[1, f : f + 1, :]
        rest = jnp.concatenate([scale, shift], axis=0)
        parts = []
        for _ in range(3):
            part = rest.astype(bf16)
            parts.append(part)
            rest = rest - part.astype(f32)
        vectors = jnp.concatenate(
            [p.astype(f32) for p in parts] + [jnp.zeros((2, width), f32)], axis=0
        ).astype(bf16)
        part = jnp.dot(
            vectors, out_ref[f * width : (f + 1) * width, :], preferred_element_type=f32
        )
        total = part if total is None else total + part
    vec_ref[0:2, :] = total[0:2] + total[2:4] + total[4:6]


def fold(values):
    width = values.shape[1]
    if width % LANES:
        return jnp.sum(values, axis=1, keepdims=True)
    return functools.reduce(
        jnp.add, [values[:, i : i + LANES] for i in range(0, width, LANES)]
    )


def slot_place(sizes, step, u):
    _, n_seq, _, n_tp = sizes
    source = ring_source(n_seq, lax.axis_index("seq"), step)
    return source * n_tp + back(lax.axis_index("tp"), u, n_tp)


def early_body(sizes, slots, table_ref, *refs):
    x_refs = refs[: len(slots)]
    y_ref, mean_ref, square_ref = refs[len(slots) :]
    rows, width = x_refs[0].shape
    tile = rows
    scales = [1.0 + table_ref[1, pl.ds(slot_place(sizes, *slot), 1), :] for slot in slots]

    def step(t, _):
        at = pl.ds(pl.multiple_of(t * tile, tile), tile)
        total = functools.reduce(jnp.add, [fold(x_ref[at, :].astype(f32)) for x_ref in x_refs])
        average = jnp.sum(total, axis=1, keepdims=True) / (len(slots) * width)
        total = None
        for s, x_ref in enumerate(x_refs):
            centred = x_ref[at, :].astype(f32) - average
            y_ref[s, at, :] = (centred * scales[s]).astype(bf16)
            part = fold(centred * centred)
            total = part if total is None else total + part
        mean_ref[at, :] = jnp.broadcast_to(average, (tile, LANES))
        square_ref[at, :] = jnp.broadcast_to(
            jnp.sum(total, axis=1, keepdims=True), (tile, LANES)
        )
        return 0

    lax.fori_loop(0, rows // tile, step, 0)


def project_body(sizes, early, last, table_ref, w_ref, vec_ref, y_ref, mean_ref, square_ref, *refs):
    x_refs = refs[: len(last)]
    q_ref, kv_ref, buf = refs[len(last) :]
    _, width = x_refs[0].shape
    head = q_ref.shape[1]
    features = (len(early) + len(last)) * width
    centre = mean_ref[:, 0:1]
    total, squares = None, None
    for s, x_ref in enumerate(x_refs):
        scale = 1.0 + table_ref[1, pl.ds(slot_place(sizes, *last[s]), 1), :]
        centred = x_ref[...].astype(f32) - centre
        buf[s] = (centred * scale).astype(bf16)
        part, square = fold(centred), fold(centred * centred)
        total = part if total is None else total + part
        squares = square if squares is None else squares + square
    delta = jnp.sum(total, axis=1, keepdims=True) / features
    spread = (square_ref[:, 0:1] + jnp.sum(squares, axis=1, keepdims=True)) / features
    inverse = lax.rsqrt(spread - delta * delta + epsilon)
    acc = None
    for s, slot in enumerate(early + last):
        first = pl.multiple_of(slot_place(sizes, *slot) * width, width)
        values = y_ref[s] if s < len(early) else buf[s - len(early)]
        part = jnp.dot(values, w_ref[pl.ds(first, width), :], preferred_element_type=f32)
        acc = part if acc is None else acc + part
    result = ((acc - delta * vec_ref[0:1, :]) * inverse + vec_ref[1:2, :]).astype(bf16)
    q_ref[...] = result[:, :head]
    kv_ref[...] = result[:, head:]


def attend_body(sizes, q_count, kv_count, factor, first, last, padded, *refs):
    q_refs = refs[:q_count]
    kv_refs = refs[q_count : q_count + kv_count]
    refs = refs[q_count + kv_count :]
    if not first:
        old_refs, refs = refs[:3], refs[3:]
    row = 0
    for q_ref in q_refs:
        rows, head = q_ref.shape
        at = slice(row, row + rows)
        queries = q_ref[...]
        scores = [
            lax.dot_general(
                queries,
                kv_ref[:, :head],
                (((1,), (1,)), ((), ())),
                preferred_element_type=f32,
            )
            * factor
            for kv_ref in kv_refs
        ]
        largest = jnp.max(functools.reduce(jnp.maximum, scores), axis=1, keepdims=True)
        if not first:
            old = old_refs[0][at, 0:1]
            largest = jnp.maximum(largest, old)
            rescale = jnp.exp(old - largest)
        total, weighted = None, None
        for block, kv_ref in zip(scores, kv_refs):
            weights = jnp.exp(block - largest)
            part = jnp.dot(
                weights.astype(bf16), kv_ref[:, head:], preferred_element_type=f32
            )
            weighted = part if weighted is None else weighted + part
            total = weights if total is None else total + weights
        total = jnp.sum(total, axis=1, keepdims=True)
        if not first:
            total = total + old_refs[1][at, 0:1] * rescale
            weighted = weighted + old_refs[2][at, :] * rescale
        if last:
            own = lax.axis_index("seq") * sizes[3] + lax.axis_index("tp")
            live = own < sizes[1] * sizes[3] - padded[0]
            refs[0][at, :] = jnp.where(live, weighted / total, 0.0).astype(bf16)
        else:
            refs[0][at, :] = jnp.broadcast_to(largest, (rows, LANES))
            refs[1][at, :] = jnp.broadcast_to(total, (rows, LANES))
            refs[2][at, :] = weighted
        row += rows


def output_early_body(sizes, slots, last_step, sources, *refs):
    n_tp = sizes[3]
    att_refs = refs[: len(slots)]
    w_refs = refs[len(slots) : len(slots) + len(sources)]
    acc_ref, rest_ref, buf = refs[len(slots) + len(sources) :]
    for w_ref, source in zip(w_refs, sources):
        buf[source()] = w_ref[...]
    seq_at = lax.axis_index("seq")
    acc = None
    head = att_refs[0].shape[1]
    for i in range(0, len(slots), n_tp):
        count = len(slots[i : i + n_tp])
        values = jnp.concatenate([r[...] for r in att_refs[i : i + n_tp]], axis=1)
        weight = buf[ring_source(sizes[1], seq_at, slots[i][0])][: count * head]
        part = jnp.dot(values, weight, preferred_element_type=f32)
        acc = part if acc is None else acc + part
    acc_ref[...] = acc
    rest_ref[...] = buf[ring_source(sizes[1], seq_at, last_step)][head:]


def output_body(sizes, table_ref, acc_ref, w_ref, *refs):
    *att_refs, out_ref = refs
    values = jnp.concatenate([r[...] for r in att_refs], axis=1)
    summed = acc_ref[...] + jnp.dot(values, w_ref[...], preferred_element_type=f32)
    own = lax.axis_index("seq") * sizes[3] + lax.axis_index("tp")
    out_ref[...] = (summed * table_ref[2, pl.ds(own, 1), :]).astype(bf16)


def shares_weights(sizes):
    n_grp, _, n_blk, _ = sizes
    return n_grp == 2 and n_blk == 2


def shares_columns(sizes):
    n_grp, n_seq, n_blk, _ = sizes
    return n_grp == n_seq // n_blk


def body(sizes, *arrays):
    return block(sizes, *arrays)


def block(sizes, tokens, timestep, padded_heads, modulation, qkv_weight, out_weight):
    n_grp, n_seq, n_blk, n_tp = sizes
    slices = n_seq * n_tp
    own_width = tokens.shape[1]
    half = tokens.shape[0] // 2
    head = out_weight.shape[0]
    order = folded_order(n_seq)
    forward, backward = ring_pairs(order), ring_pairs(order, -1)
    DMA = pltpu.SemaphoreType.DMA

    by_two = shares_weights(sizes)
    cut = kernel(
        functools.partial(split_body, by_two),
        [((half, own_width), bf16)] * 2 + [(qkv_weight.shape[1:], bf16)] * (2 if by_two else 0),
        [(tokens, "far"), (qkv_weight, "far")],
        [DMA((4,))],
    )
    current = list(cut[:2])
    slots = [{}, {}]
    for step in range(n_seq):
        for chunk in range(2):
            if step:
                current[chunk] = lax.ppermute(current[chunk], "seq", forward)
            slots[chunk][step, 0] = current[chunk]
            for u in range(1, n_tp):
                slots[chunk][step, u] = lax.ppermute(current[chunk], "tp", rotation(n_tp, u))

    (table,) = kernel(
        table_body,
        [((3, slices, own_width), f32)],
        [(timestep, "smem"), (jnp.swapaxes(modulation, 0, 1), "near")],
    )

    parts, pieces = [(qkv_weight, "far")], [(3, lambda b: b, None)]
    if by_two:
        relayed, direct = cut[2:]
        first = lax.ppermute(relayed, "blk", rotation(2, 1))
        second = lax.ppermute(direct, "blk", rotation(2, 1))
        third = lax.ppermute(first, "group", rotation(2, 1))
        parts += [(first, "near"), (second, "near"), (third, "near")]
        pieces += [
            (1, lambda b: 1 - b, lambda g: g),
            (1, lambda b: 1 - b, lambda g: 2),
            (1, lambda b: 1 - b, lambda g: 1 - g),
        ]
    else:
        for j in range(1, n_blk):
            parts.append((lax.ppermute(qkv_weight, "blk", rotation(n_blk, j)), "near"))
            pieces.append((3, lambda b, j=j: back(b, j, n_blk), None))
    weight, vectors = kernel(
        functools.partial(merge_body, pieces),
        [((slices * own_width, 3 * head), bf16), ((8, 3 * head), f32)],
        [(table, "near")] + parts,
        [DMA((len(pieces), 3))],
    )

    n_low = n_seq // n_blk
    shared = shares_columns(sizes)
    o_parts, o_sources = [], []

    def source_of(k3, shift):
        def source():
            low = lax.rem(lax.axis_index("seq"), n_low)
            s = back(lax.axis_index("group"), -shift, n_grp) if shared else shift
            low = lax.rem(low - s + n_low, n_low)
            high = lax.rem(lax.axis_index("blk") - k3 - low + (n_low + 1) * n_blk, n_blk)
            return high * n_low + low

        return source

    for k1 in range(1 if shared else n_low):
        received = list(
            kernel(
                functools.partial(columns_body, sizes, None if shared else k1),
                [((head, own_width), bf16)] * n_tp,
                [(out_weight, "far")],
                [DMA((n_tp,))],
            )
            if own_width % LANES == 0
            else [
                lax.dynamic_slice(
                    out_weight,
                    (0, column_of(sizes, None if shared else k1, u, own_width)),
                    (head, own_width),
                )
                for u in range(n_tp)
            ]
        )
        for u in range(1, n_tp):
            received[u] = lax.ppermute(received[u], "tp", rotation(n_tp, u))
        (rows,) = kernel(
            stack_body, [((n_tp * head, own_width), bf16)], [(x, "near") for x in received]
        )
        for k3 in range(1 if shared else n_blk):
            pairs = []
            for g in range(n_grp):
                for z in range(n_seq):
                    for b in range(n_blk):
                        l2 = (z % n_low + (g if shared else k1)) % n_low
                        x2 = (z // n_low + z % n_low + k3) % n_blk
                        target = (g * n_seq + b * n_low + l2) * n_blk + x2
                        pairs.append(((g * n_seq + z) * n_blk + b, target))
            arrived = lax.ppermute(rows, ("group", "seq", "blk"), pairs)
            o_parts.append(arrived)
            o_sources.append(source_of(k3, 0 if shared else k1))
        if shared:
            for g in range(n_grp):
                for j in range(n_blk):
                    if g or j:
                        swap = [
                            (p * n_blk + b, (p + g) % n_grp * n_blk + (b + j) % n_blk)
                            for p in range(n_grp)
                            for b in range(n_blk)
                        ]
                        o_parts.append(lax.ppermute(arrived, ("group", "blk"), swap))
                        o_sources.append(source_of(j, -g))

    early = [(s, u) for s in range(n_seq - 1) for u in range(n_tp)]
    last = [(n_seq - 1, u) for u in range(n_tp)]
    starts = [
        kernel(
            functools.partial(early_body, sizes, early),
            [
                ((len(early), half, own_width), bf16),
                ((half, LANES), f32),
                ((half, LANES), f32),
            ],
            [(table, "near")] + [(slots[chunk][slot], "near") for slot in early],
        )
        for chunk in range(2)
    ]
    q_parts, kv_own, kv_rest = [], [], []
    for chunk in range(2):
        q, kv = kernel(
            functools.partial(project_body, sizes, early, last),
            [((half, head), bf16), ((half, 2 * head), bf16)],
            [(x, "near") for x in (table, weight, vectors, *starts[chunk])]
            + [(slots[chunk][slot], "near") for slot in last],
            [pltpu.VMEM((len(last), half, own_width), bf16)],
        )
        q_parts.append(q)
        kv_own.append(kv)
        for j in range(1, n_blk):
            kv_rest.append(lax.ppermute(kv, "blk", rotation(n_blk, j)))

    factor = 1.0 / math.sqrt(head)
    state = kernel(
        functools.partial(attend_body, sizes, 2, len(kv_own), factor, True, False),
        [((2 * half, LANES), f32), ((2 * half, LANES), f32), ((2 * half, head), f32)],
        [(padded_heads, "smem")] + [(x, "near") for x in q_parts + kv_own],
    )
    (masked,) = kernel(
        functools.partial(attend_body, sizes, 2, len(kv_rest), factor, False, True),
        [((2 * half, head), bf16)],
        [(padded_heads, "smem")] + [(x, "near") for x in (*q_parts, *kv_rest, *state)],
    )

    att = {(0, 0): masked}
    up, down = masked, masked
    last_step = n_seq // 2
    for step in range(1, last_step + 1):
        up = att[step, 0] = lax.ppermute(up, "seq", forward)
        if n_seq - step > step:
            down = att[n_seq - step, 0] = lax.ppermute(down, "seq", backward)
    for step in range(n_seq):
        for u in range(1, n_tp):
            att[step, u] = lax.ppermute(att[step, 0], "tp", rotation(n_tp, u))
    first_slots = [(s, u) for s in range(n_seq) if s != last_step for u in range(n_tp)]
    first_slots.append((last_step, 0))
    acc, rest = kernel(
        functools.partial(output_early_body, sizes, first_slots, last_step, o_sources),
        [((2 * half, own_width), f32), (((n_tp - 1) * head, own_width), bf16)],
        [(att[slot], "near") for slot in first_slots] + [(x, "near") for x in o_parts],
        [pltpu.VMEM((n_seq, n_tp * head, own_width), bf16)],
    )
    return pl.pallas_call(
        functools.partial(output_body, sizes),
        out_shape=jax.ShapeDtypeStruct((2 * half, own_width), bf16),
        in_specs=[VMEM] * (2 + n_tp),
        out_specs=VMEM,
        compiler_params=PARAMS,
        name="output",
    )(near(table), near(acc), near(rest), *[near(att[last_step, u]) for u in range(1, n_tp)])


def solution(mesh):
    sizes = tuple(mesh.shape[a] for a in ("group", "seq", "blk", "tp"))
    return jax.shard_map(
        functools.partial(body, sizes),
        mesh=mesh,
        in_specs=(
            P(("group", "blk"), ("seq", "tp")),
            P("group"),
            P("group"),
            P(),
            P(None, "blk", ("seq", "tp")),
            P(("seq", "tp"), "blk"),
        ),
        out_specs=P(("group", "blk"), ("seq", "tp")),
        check_vma=False,
    )
```

```python
import functools
import math

import jax
import jax.numpy as jnp
from jax import lax
from jax.experimental import pallas as pl
from jax.experimental.pallas import tpu as pltpu
from jax.sharding import PartitionSpec as P

epsilon = 1e-06
ANY = pl.BlockSpec(memory_space=pl.ANY)
VMEM = pl.BlockSpec(memory_space=pltpu.VMEM)
SMEM = pl.BlockSpec(memory_space=pltpu.SMEM)
PARAMS = pltpu.CompilerParams(vmem_limit_bytes=16 << 20)
LANES = 128
VECTORS = 16
f32, bf16 = jnp.float32, jnp.bfloat16


def folded_order(count):
    return list(range(1, count, 2)) + list(range(0, count, 2))[::-1]


def ring_pairs(order, step=1):
    count = len(order)
    return [(order[i], order[(i + step) % count]) for i in range(count)]


def ring_source(count, at, step):
    order = folded_order(count)
    source = 0
    for i, device in enumerate(order):
        source = jnp.where(at == device, order[(i - step) % count], source)
    return source


def rotation(count, offset):
    return [(i, (i + offset) % count) for i in range(count)]


def back(at, offset, count):
    return lax.rem(at + count - offset, count)


def near(x):
    return pltpu.with_memory_space_constraint(x, pltpu.VMEM)


def far(x):
    return pltpu.with_memory_space_constraint(x, pltpu.HBM)


def kernel(body, outs, ins, scratch=()):
    specs = {"near": VMEM, "far": ANY, "smem": SMEM}
    places = {"near": near, "far": far, "smem": lambda x: x}
    return pl.pallas_call(
        body,
        out_shape=tuple(pltpu.VMEM(shape, dtype) for shape, dtype in outs),
        in_specs=[specs[where] for _, where in ins],
        out_specs=tuple(VMEM for _ in outs),
        scratch_shapes=list(scratch),
        compiler_params=PARAMS,
    )(*[places[where](x) for x, where in ins])


def run_copies(copies):
    for copy in copies:
        copy.start()
    for copy in copies:
        copy.wait()


def split_body(shared, x_ref, w_ref, top_ref, bottom_ref, *refs):
    half = top_ref.shape[0]
    sem = refs[-1]
    copies = [
        pltpu.make_async_copy(x_ref.at[pl.ds(0, half)], top_ref, sem.at[0]),
        pltpu.make_async_copy(x_ref.at[pl.ds(half, half)], bottom_ref, sem.at[1]),
    ]
    if shared:
        plane = lax.axis_index("group")
        copies += [
            pltpu.make_async_copy(w_ref.at[plane], refs[0], sem.at[2]),
            pltpu.make_async_copy(w_ref.at[2], refs[1], sem.at[3]),
        ]
    run_copies(copies)


def table_body(at, m_ref, out_ref, vec_ref):
    _, slices, width = out_ref.shape
    rows = [m_ref[i, pl.ds(at[0], 1), :] for i in range(3)]
    for f in range(slices):
        cut = [row[:, f * width : (f + 1) * width] for row in rows]
        for i in range(3):
            out_ref[i, f : f + 1, :] = cut[i]
        rest = jnp.concatenate([1.0 + cut[1], cut[0]], axis=0)
        parts = []
        for _ in range(3):
            parts.append(rest.astype(bf16).astype(f32))
            rest = rest - parts[-1]
        parts.append(jnp.zeros((VECTORS - 6, width), f32))
        vec_ref[f] = jnp.concatenate(parts, axis=0).astype(bf16)


def column_of(sizes, shift, u, width):
    _, n_seq, n_blk, n_tp = sizes
    n_low = n_seq // n_blk
    if shift is None:
        shift = lax.axis_index("group")
    place = lax.rem(lax.rem(lax.axis_index("seq"), n_low) + shift, n_low)
    core = lax.rem(lax.axis_index("tp") + u, n_tp)
    return pl.multiple_of((place * n_tp + core) * width, math.gcd(width, LANES))


def columns_body(sizes, shift, w_ref, *refs):
    *out_refs, sem = refs
    width = out_refs[0].shape[1]
    run_copies(
        [
            pltpu.make_async_copy(
                w_ref.at[:, pl.ds(column_of(sizes, shift, u, width), width)], out_ref, sem.at[u]
            )
            for u, out_ref in enumerate(out_refs)
        ]
    )


def stack_body(*refs):
    *in_refs, out_ref = refs
    rows = in_refs[0].shape[0]
    for i, in_ref in enumerate(in_refs):
        out_ref[i * rows : (i + 1) * rows, :] = in_ref[...]


def merge_body(pieces, *refs):
    w_refs = refs[: len(pieces)]
    out_ref, sem = refs[len(pieces) :]
    blk_at, grp_at = lax.axis_index("blk"), lax.axis_index("group")
    copies = []
    for j, (planes, offset, column) in enumerate(pieces):
        rows, head = w_refs[j].shape[-2:]
        first = pl.multiple_of(back(blk_at, offset, w_blocks(pieces)) * rows, rows)
        for i in range(planes):
            source = w_refs[j].at[i] if planes > 1 else w_refs[j]
            at = i * head if planes > 1 else pl.multiple_of(column(grp_at) * head, head)
            copies.append(
                pltpu.make_async_copy(
                    source, out_ref.at[pl.ds(first, rows), pl.ds(at, head)], sem.at[j, i]
                )
            )
    run_copies(copies)


def w_blocks(pieces):
    return 1 + max(offset for _, offset, _ in pieces)


def fold(values):
    width = values.shape[1]
    if width % LANES:
        return jnp.sum(values, axis=1, keepdims=True)
    return functools.reduce(
        jnp.add, [values[:, i : i + LANES] for i in range(0, width, LANES)]
    )


def slot_place(sizes, step, u):
    _, n_seq, _, n_tp = sizes
    source = ring_source(n_seq, lax.axis_index("seq"), step)
    return source * n_tp + back(lax.axis_index("tp"), u, n_tp)


def early_body(sizes, slots, table_ref, *refs):
    x_refs = refs[: len(slots)]
    y_ref, mean_ref, square_ref = refs[len(slots) :]
    rows, width = x_refs[0].shape
    tile = rows
    scales = [1.0 + table_ref[1, pl.ds(slot_place(sizes, *slot), 1), :] for slot in slots]

    def step(t, _):
        at = pl.ds(pl.multiple_of(t * tile, tile), tile)
        total = functools.reduce(jnp.add, [fold(x_ref[at, :].astype(f32)) for x_ref in x_refs])
        average = jnp.sum(total, axis=1, keepdims=True) / (len(slots) * width)
        total = None
        for s, x_ref in enumerate(x_refs):
            centred = x_ref[at, :].astype(f32) - average
            y_ref[s, at, :] = (centred * scales[s]).astype(bf16)
            part = fold(centred * centred)
            total = part if total is None else total + part
        mean_ref[at, :] = jnp.broadcast_to(average, (tile, LANES))
        square_ref[at, :] = jnp.broadcast_to(
            jnp.sum(total, axis=1, keepdims=True), (tile, LANES)
        )
        return 0

    lax.fori_loop(0, rows // tile, step, 0)


def project_body(sizes, early, last, first, table_ref, w_ref, vec_ref, y_ref, mean_ref, square_ref, *refs):
    x_refs = refs[: len(last)]
    q_ref, kv_ref, *made_ref, buf = refs[len(last) :]
    rows, width = x_refs[0].shape
    head = q_ref.shape[1]
    features = (len(early) + len(last)) * width
    centre = mean_ref[:, 0:1]
    total, squares = None, None
    for s, x_ref in enumerate(x_refs):
        scale = 1.0 + table_ref[1, pl.ds(slot_place(sizes, *last[s]), 1), :]
        centred = x_ref[...].astype(f32) - centre
        buf[s] = (centred * scale).astype(bf16)
        part, square = fold(centred), fold(centred * centred)
        total = part if total is None else total + part
        squares = square if squares is None else squares + square
    delta = jnp.sum(total, axis=1, keepdims=True) / features
    spread = (square_ref[:, 0:1] + jnp.sum(squares, axis=1, keepdims=True)) / features
    inverse = lax.rsqrt(spread - delta * delta + epsilon)
    acc = None
    for s, slot in enumerate(early + last):
        place = slot_place(sizes, *slot)
        values = y_ref[s] if s < len(early) else buf[s - len(early)]
        if first:
            values = jnp.concatenate([values, vec_ref[place]], axis=0)
        at = pl.ds(pl.multiple_of(place * width, width), width)
        part = jnp.dot(values, w_ref[at, :], preferred_element_type=f32)
        acc = part if acc is None else acc + part
    if first:
        vectors = acc[rows : rows + 2] + acc[rows + 2 : rows + 4] + acc[rows + 4 : rows + 6]
        made_ref[0][0:2] = vectors
    else:
        vectors = vec_ref[0:2]
    result = ((acc[:rows] - delta * vectors[0:1]) * inverse + vectors[1:2]).astype(bf16)
    q_ref[...] = result[:, :head]
    kv_ref[...] = result[:, head:]


def attend_body(sizes, q_count, kv_count, factor, first, last, padded, *refs):
    q_refs = refs[:q_count]
    kv_refs = refs[q_count : q_count + kv_count]
    refs = refs[q_count + kv_count :]
    if not first:
        old_refs, refs = refs[:3], refs[3:]
    row = 0
    for q_ref in q_refs:
        rows, head = q_ref.shape
        at = slice(row, row + rows)
        queries = q_ref[...]
        scores = [
            lax.dot_general(
                queries,
                kv_ref[:, :head],
                (((1,), (1,)), ((), ())),
                preferred_element_type=f32,
            )
            * factor
            for kv_ref in kv_refs
        ]
        largest = jnp.max(functools.reduce(jnp.maximum, scores), axis=1, keepdims=True)
        if not first:
            old = old_refs[0][at, 0:1]
            largest = jnp.maximum(largest, old)
            rescale = jnp.exp(old - largest)
        total, weighted = None, None
        for block, kv_ref in zip(scores, kv_refs):
            weights = jnp.exp(block - largest)
            part = jnp.dot(
                weights.astype(bf16), kv_ref[:, head:], preferred_element_type=f32
            )
            weighted = part if weighted is None else weighted + part
            total = weights if total is None else total + weights
        total = jnp.sum(total, axis=1, keepdims=True)
        if not first:
            total = total + old_refs[1][at, 0:1] * rescale
            weighted = weighted + old_refs[2][at, :] * rescale
        if last:
            own = lax.axis_index("seq") * sizes[3] + lax.axis_index("tp")
            live = own < sizes[1] * sizes[3] - padded[0]
            refs[0][at, :] = jnp.where(live, weighted / total, 0.0).astype(bf16)
        else:
            refs[0][at, :] = jnp.broadcast_to(largest, (rows, LANES))
            refs[1][at, :] = jnp.broadcast_to(total, (rows, LANES))
            refs[2][at, :] = weighted
        row += rows


def output_early_body(sizes, slots, last_step, sources, *refs):
    n_tp = sizes[3]
    att_refs = refs[: len(slots)]
    w_refs = refs[len(slots) : len(slots) + len(sources)]
    acc_ref, rest_ref, buf = refs[len(slots) + len(sources) :]
    for w_ref, source in zip(w_refs, sources):
        buf[source()] = w_ref[...]
    seq_at = lax.axis_index("seq")
    acc = None
    head = att_refs[0].shape[1]
    for i in range(0, len(slots), n_tp):
        count = len(slots[i : i + n_tp])
        values = jnp.concatenate([r[...] for r in att_refs[i : i + n_tp]], axis=1)
        weight = buf[ring_source(sizes[1], seq_at, slots[i][0])][: count * head]
        part = jnp.dot(values, weight, preferred_element_type=f32)
        acc = part if acc is None else acc + part
    acc_ref[...] = acc
    rest_ref[...] = buf[ring_source(sizes[1], seq_at, last_step)][head:]


def output_body(sizes, table_ref, acc_ref, w_ref, *refs):
    *att_refs, out_ref = refs
    values = jnp.concatenate([r[...] for r in att_refs], axis=1)
    summed = acc_ref[...] + jnp.dot(values, w_ref[...], preferred_element_type=f32)
    own = lax.axis_index("seq") * sizes[3] + lax.axis_index("tp")
    out_ref[...] = (summed * table_ref[2, pl.ds(own, 1), :]).astype(bf16)


def shares_weights(sizes):
    n_grp, _, n_blk, _ = sizes
    return n_grp == 2 and n_blk == 2


def shares_columns(sizes):
    n_grp, n_seq, n_blk, _ = sizes
    return n_grp == n_seq // n_blk


def body(sizes, *arrays):
    return block(sizes, *arrays)


def block(sizes, tokens, timestep, padded_heads, modulation, qkv_weight, out_weight):
    n_grp, n_seq, n_blk, n_tp = sizes
    slices = n_seq * n_tp
    own_width = tokens.shape[1]
    half = tokens.shape[0] // 2
    head = out_weight.shape[0]
    order = folded_order(n_seq)
    forward, backward = ring_pairs(order), ring_pairs(order, -1)
    DMA = pltpu.SemaphoreType.DMA

    by_two = shares_weights(sizes)
    cut = kernel(
        functools.partial(split_body, by_two),
        [((half, own_width), bf16)] * 2 + [(qkv_weight.shape[1:], bf16)] * (2 if by_two else 0),
        [(tokens, "far"), (qkv_weight, "far")],
        [DMA((4,))],
    )
    current = list(cut[:2])
    slots = [{}, {}]
    for step in range(n_seq):
        for chunk in range(2):
            if step:
                current[chunk] = lax.ppermute(current[chunk], "seq", forward)
            slots[chunk][step, 0] = current[chunk]
            for u in range(1, n_tp):
                slots[chunk][step, u] = lax.ppermute(current[chunk], "tp", rotation(n_tp, u))

    table, vectors = kernel(
        table_body,
        [((3, slices, own_width), f32), ((slices, VECTORS, own_width), bf16)],
        [(timestep, "smem"), (jnp.swapaxes(modulation, 0, 1), "near")],
    )

    parts, pieces = [(qkv_weight, "far")], [(3, 0, None)]
    if by_two:
        relayed, direct = cut[2:]
        first = lax.ppermute(relayed, "blk", rotation(2, 1))
        second = lax.ppermute(direct, "blk", rotation(2, 1))
        third = lax.ppermute(first, "group", rotation(2, 1))
        parts += [(first, "near"), (second, "near"), (third, "near")]
        pieces += [
            (1, 1, lambda g: g),
            (1, 1, lambda g: 2),
            (1, 1, lambda g: 1 - g),
        ]
    else:
        for j in range(1, n_blk):
            parts.append((lax.ppermute(qkv_weight, "blk", rotation(n_blk, j)), "near"))
            pieces.append((3, j, None))
    (weight,) = kernel(
        functools.partial(merge_body, pieces),
        [((slices * own_width, 3 * head), bf16)],
        parts,
        [DMA((len(pieces), 3))],
    )

    n_low = n_seq // n_blk
    shared = shares_columns(sizes)
    o_parts, o_sources = [], []

    def source_of(k3, shift):
        def source():
            low = lax.rem(lax.axis_index("seq"), n_low)
            s = back(lax.axis_index("group"), -shift, n_grp) if shared else shift
            low = lax.rem(low - s + n_low, n_low)
            own = lax.div(lax.axis_index("seq"), n_low)
            high = lax.rem(lax.axis_index("blk") - own - k3 - low + (n_low + 2) * n_blk, n_blk)
            return high * n_low + low

        return source

    for k1 in range(1 if shared else n_low):
        received = list(
            kernel(
                functools.partial(columns_body, sizes, None if shared else k1),
                [((head, own_width), bf16)] * n_tp,
                [(out_weight, "far")],
                [DMA((n_tp,))],
            )
            if own_width % LANES == 0
            else [
                lax.dynamic_slice(
                    out_weight,
                    (0, column_of(sizes, None if shared else k1, u, own_width)),
                    (head, own_width),
                )
                for u in range(n_tp)
            ]
        )
        for u in range(1, n_tp):
            received[u] = lax.ppermute(received[u], "tp", rotation(n_tp, u))
        (rows,) = kernel(
            stack_body, [((n_tp * head, own_width), bf16)], [(x, "near") for x in received]
        )
        for k3 in range(1 if shared else n_blk):
            hops, pairs, whole = [], [], []
            for g in range(n_grp):
                for z in range(n_seq):
                    for b in range(n_blk):
                        l2 = (z % n_low + (g if shared else k1)) % n_low
                        x2 = (b + z // n_low + z % n_low + k3) % n_blk
                        there = (g * n_seq + z) * n_blk
                        target = (g * n_seq + b * n_low + l2) * n_blk + x2
                        hops.append((z * n_blk + b, z * n_blk + x2))
                        pairs.append((there + x2, target))
                        whole.append((there + b, target))
            if shared:
                moved = lax.ppermute(rows, ("seq", "blk"), hops[: n_seq * n_blk])
                arrived = lax.ppermute(moved, ("group", "seq", "blk"), pairs)
            else:
                arrived = lax.ppermute(rows, ("group", "seq", "blk"), whole)
            o_parts.append(arrived)
            o_sources.append(source_of(k3, 0 if shared else k1))
        if shared:
            for g in range(n_grp):
                for j in range(n_blk):
                    if g or j:
                        swap = [
                            (p * n_blk + b, (p + g) % n_grp * n_blk + (b + j) % n_blk)
                            for p in range(n_grp)
                            for b in range(n_blk)
                        ]
                        o_parts.append(lax.ppermute(arrived, ("group", "blk"), swap))
                        o_sources.append(source_of(j, -g))

    early = [(s, u) for s in range(n_seq - 1) for u in range(n_tp)]
    last = [(n_seq - 1, u) for u in range(n_tp)]
    starts = [
        kernel(
            functools.partial(early_body, sizes, early),
            [
                ((len(early), half, own_width), bf16),
                ((half, LANES), f32),
                ((half, LANES), f32),
            ],
            [(table, "near")] + [(slots[chunk][slot], "near") for slot in early],
        )
        for chunk in range(2)
    ]
    q_parts, kv_own, kv_rest = [], [], []
    for chunk in range(2):
        q, kv, *made = kernel(
            functools.partial(project_body, sizes, early, last, chunk == 0),
            [((half, head), bf16), ((half, 2 * head), bf16)]
            + [((8, 3 * head), f32)] * (chunk == 0),
            [(x, "near") for x in (table, weight, vectors, *starts[chunk])]
            + [(slots[chunk][slot], "near") for slot in last],
            [pltpu.VMEM((len(last), half, own_width), bf16)],
        )
        if made:
            (vectors,) = made
        q_parts.append(q)
        kv_own.append(kv)
        for j in range(1, n_blk):
            kv_rest.append(lax.ppermute(kv, "blk", rotation(n_blk, j)))

    factor = 1.0 / math.sqrt(head)
    state = kernel(
        functools.partial(attend_body, sizes, 2, len(kv_own), factor, True, False),
        [((2 * half, LANES), f32), ((2 * half, LANES), f32), ((2 * half, head), f32)],
        [(padded_heads, "smem")] + [(x, "near") for x in q_parts + kv_own],
    )
    (masked,) = kernel(
        functools.partial(attend_body, sizes, 2, len(kv_rest), factor, False, True),
        [((2 * half, head), bf16)],
        [(padded_heads, "smem")] + [(x, "near") for x in (*q_parts, *kv_rest, *state)],
    )

    att = {(0, 0): masked}
    up, down = masked, masked
    last_step = n_seq // 2
    for step in range(1, last_step + 1):
        up = att[step, 0] = lax.ppermute(up, "seq", forward)
        if n_seq - step > step:
            down = att[n_seq - step, 0] = lax.ppermute(down, "seq", backward)
    for step in range(n_seq):
        for u in range(1, n_tp):
            att[step, u] = lax.ppermute(att[step, 0], "tp", rotation(n_tp, u))
    first_slots = [(s, u) for s in range(n_seq) if s != last_step for u in range(n_tp)]
    first_slots.append((last_step, 0))
    acc, rest = kernel(
        functools.partial(output_early_body, sizes, first_slots, last_step, o_sources),
        [((2 * half, own_width), f32), (((n_tp - 1) * head, own_width), bf16)],
        [(att[slot], "near") for slot in first_slots] + [(x, "near") for x in o_parts],
        [pltpu.VMEM((n_seq, n_tp * head, own_width), bf16)],
    )
    return pl.pallas_call(
        functools.partial(output_body, sizes),
        out_shape=jax.ShapeDtypeStruct((2 * half, own_width), bf16),
        in_specs=[VMEM] * (2 + n_tp),
        out_specs=VMEM,
        compiler_params=PARAMS,
        name="output",
    )(near(table), near(acc), near(rest), *[near(att[last_step, u]) for u in range(1, n_tp)])


def solution(mesh):
    sizes = tuple(mesh.shape[a] for a in ("group", "seq", "blk", "tp"))
    return jax.shard_map(
        functools.partial(body, sizes),
        mesh=mesh,
        in_specs=(
            P(("group", "blk"), ("seq", "tp")),
            P("group"),
            P("group"),
            P(),
            P(None, "blk", ("seq", "tp")),
            P(("seq", "tp"), "blk"),
        ),
        out_specs=P(("group", "blk"), ("seq", "tp")),
        check_vma=False,
    )
```
